8 devices in a mesh: data: 1 (over z), model: 8 (over y, x, core).
Axes of the slice: x: 2, y: 2, z: 1, core: 2. Of those that a mesh axis runs over, the one named last changes fastest.
Arguments:
- x_in: bfloat16 [1, 4096, 5120], P('data')
- seg_ids: int32 [1, 4096], P('data')
- gain_one: bfloat16 [5120], replicated
- w_qkv: bfloat16 [5120, 15360], P(None, 'model')
- w_out: bfloat16 [40, 128, 5120], P('model')
- gain_two: bfloat16 [5120], replicated
- w_up: bfloat16 [5120, 20480], P(None, 'model')
- w_down: bfloat16 [20480, 5120], P('model')
- d_y: bfloat16 [1, 4096, 5120], P('data')
Outputs:
- output 1: bfloat16 [1, 4096, 5120], P('data')
- output 2: bfloat16 [1, 4096, 5120], P('data')
- output 3: bfloat16 [5120, 15360], P('data', 'model')
- output 4: bfloat16 [40, 128, 5120], P(('data', 'model'))
- output 5: bfloat16 [5120, 20480], P('data', 'model')
- output 6: bfloat16 [20480, 5120], P(('data', 'model'))
- output 7: bfloat16 [5120], P('data')
- output 8: bfloat16 [5120], P('data')
All inputs are finite; a program needn't handle non-finite values.
Results may differ from the reference program's by a relative error of at most 0.02.
Values are sent between devices in bfloat16 or wider.
A program may use at most 1.25 GiB of HBM per device.

```python
import jax
import jax.numpy as jnp
from jax import lax

BATCH_ROWS = 1
SEQ_LEN = 4096
MODEL_DIM = 5120
NUM_HEADS = 40
HEAD_DIM = 128
FFN_DIM = 20480
LN_EPS = 1e-5
TOKEN_COUNT = BATCH_ROWS * SEQ_LEN
QKV_WIDTH = 3 * NUM_HEADS * HEAD_DIM
INNER_WIDTH = NUM_HEADS * HEAD_DIM


def draw_segments(seg_key):
    seg_keys = jax.random.split(seg_key, 3)
    rate_table = jnp.array([0, 2, 8, 32], jnp.int32)
    row_rate = rate_table[jax.random.randint(seg_keys[0], (BATCH_ROWS,), 0, 4)]
    pos_draws = jax.random.randint(seg_keys[1], (BATCH_ROWS, SEQ_LEN), 0, SEQ_LEN)
    forced_pos = jax.random.randint(seg_keys[2], (BATCH_ROWS,), 1, SEQ_LEN)
    positions = jnp.arange(SEQ_LEN, dtype=jnp.int32)
    breaks = ((pos_draws < row_rate[:, None]) | (positions[None, :] == forced_pos[:, None])).astype(jnp.int32)
    breaks = breaks.at[:, 0].set(0)
    return jnp.cumsum(breaks, axis=1).astype(jnp.int32)


def setup_inputs(seed: int = 0, part: int = 0) -> dict:
    base_key = jax.random.key(seed)
    part_key = jax.random.fold_in(base_key, part)
    weight_keys = jax.random.split(base_key, 6)
    part_keys = jax.random.split(part_key, 4)
    x_in = jax.random.normal(part_keys[0], (BATCH_ROWS, SEQ_LEN, MODEL_DIM), jnp.float32)
    seg_ids = draw_segments(part_keys[1])
    gain_one = 1.0 + 0.3 * jax.random.normal(weight_keys[0], (MODEL_DIM,), jnp.float32)
    gain_two = 1.0 + 0.3 * jax.random.normal(weight_keys[1], (MODEL_DIM,), jnp.float32)
    w_qkv = jax.random.normal(weight_keys[2], (MODEL_DIM, QKV_WIDTH), jnp.float32) * (1.5 * MODEL_DIM ** -0.5)
    w_out = jax.random.normal(weight_keys[3], (NUM_HEADS, HEAD_DIM, MODEL_DIM), jnp.float32) * INNER_WIDTH ** -0.5
    w_up = jax.random.normal(weight_keys[4], (MODEL_DIM, FFN_DIM), jnp.float32) * MODEL_DIM ** -0.5
    w_down = jax.random.normal(weight_keys[5], (FFN_DIM, MODEL_DIM), jnp.float32) * FFN_DIM ** -0.5
    d_y = jax.random.normal(part_keys[3], (BATCH_ROWS, SEQ_LEN, MODEL_DIM), jnp.float32)
    return {'x_in': x_in.astype(jnp.bfloat16), 'seg_ids': seg_ids, 'gain_one': gain_one.astype(jnp.bfloat16), 'w_qkv': w_qkv.astype(jnp.bfloat16), 'w_out': w_out.astype(jnp.bfloat16), 'gain_two': gain_two.astype(jnp.bfloat16), 'w_up': w_up.astype(jnp.bfloat16), 'w_down': w_down.astype(jnp.bfloat16), 'd_y': d_y.astype(jnp.bfloat16)}


def layer_norm(x_in, gain):
    x_wide = x_in.astype(jnp.float32)
    row_mean = jnp.mean(x_wide, axis=-1, keepdims=True)
    centered = x_wide - row_mean
    row_var = jnp.mean(centered * centered, axis=-1, keepdims=True)
    return (centered * lax.rsqrt(row_var + LN_EPS) * gain.astype(jnp.float32)).astype(jnp.bfloat16)


def head_attention(q_head, k_head, v_head, seg_ids):
    positions = jnp.arange(SEQ_LEN)
    allowed = (positions[:, None] >= positions[None, :])[None] & (seg_ids[:, :, None] == seg_ids[:, None, :])
    scores = jnp.einsum('bqd,bkd->bqk', q_head.astype(jnp.float32), k_head.astype(jnp.float32)) * (HEAD_DIM ** -0.5)
    scores = jnp.where(allowed, scores, -1e30)
    attn_prob = jax.nn.softmax(scores, axis=-1).astype(jnp.bfloat16)
    result = jnp.einsum('bqk,bkd->bqd', attn_prob.astype(jnp.float32), v_head.astype(jnp.float32))
    return result.astype(jnp.bfloat16)


def layer_forward(x_in, seg_ids, gain_one, w_qkv, w_out, gain_two, w_up, w_down):
    x_flat = x_in.reshape(TOKEN_COUNT, MODEL_DIM)
    normed_one = layer_norm(x_flat, gain_one)
    qkv_proj = jnp.dot(normed_one, w_qkv, preferred_element_type=jnp.float32).astype(jnp.bfloat16)
    qkv_heads = jnp.moveaxis(qkv_proj.reshape(BATCH_ROWS, SEQ_LEN, NUM_HEADS, 3, HEAD_DIM), 2, 0)

    def one_head(head_qkv):
        return head_attention(head_qkv[:, :, 0], head_qkv[:, :, 1], head_qkv[:, :, 2], seg_ids)

    attn_heads = lax.map(jax.checkpoint(one_head), qkv_heads)
    attn_flat = jnp.moveaxis(attn_heads, 0, 2).reshape(TOKEN_COUNT, INNER_WIDTH)
    proj_one = jnp.dot(attn_flat, w_out.reshape(INNER_WIDTH, MODEL_DIM), preferred_element_type=jnp.float32)
    resid = (x_flat.astype(jnp.float32) + proj_one).astype(jnp.bfloat16)
    normed_two = layer_norm(resid, gain_two)
    up_proj = jnp.dot(normed_two, w_up, preferred_element_type=jnp.float32).astype(jnp.bfloat16)
    gelu_out = jax.nn.gelu(up_proj.astype(jnp.float32), approximate=True).astype(jnp.bfloat16)
    proj_two = jnp.dot(gelu_out, w_down, preferred_element_type=jnp.float32)
    y_flat = (resid.astype(jnp.float32) + proj_two).astype(jnp.bfloat16)
    return y_flat.reshape(BATCH_ROWS, SEQ_LEN, MODEL_DIM)


def reference(x_in, seg_ids, gain_one, w_qkv, w_out, gain_two, w_up, w_down, d_y):
    def forward_fn(x_arg, g_one, wq_arg, wo_arg, g_two, wu_arg, wd_arg):
        return layer_forward(x_arg, seg_ids, g_one, wq_arg, wo_arg, g_two, wu_arg, wd_arg)

    y_out, pullback = jax.vjp(forward_fn, x_in, gain_one, w_qkv, w_out, gain_two, w_up, w_down)
    d_x, d_gain_one, d_w_qkv, d_w_out, d_gain_two, d_w_up, d_w_down = pullback(d_y)
    return (y_out, d_x, d_w_qkv, d_w_out, d_w_up, d_w_down, d_gain_one, d_gain_two)
```

```python
import functools

import jax
import jax.numpy as jnp
from jax import lax
from jax.experimental import pallas as pl
from jax.experimental.pallas import tpu as pltpu
from jax.sharding import PartitionSpec as P

LN_EPS = 1e-5
LOG2_E = 1.4426950408889634
MASKED = -1e30
F32 = jnp.float32
BF16 = jnp.bfloat16


def layer_norm(x_in, gain):
    x_wide = x_in.astype(F32)
    row_mean = jnp.mean(x_wide, axis=-1, keepdims=True)
    centered = x_wide - row_mean
    row_var = jnp.mean(centered * centered, axis=-1, keepdims=True)
    return (centered * lax.rsqrt(row_var + LN_EPS) * gain.astype(F32)).astype(BF16)


def gelu_tanh(up_proj):
    return jax.nn.gelu(up_proj.astype(F32), approximate=True).astype(BF16)


def dot32(lhs, rhs, lhs_dim, rhs_dim):
    return lax.dot_general(lhs, rhs, (((lhs_dim,), (rhs_dim,)), ((), ())), preferred_element_type=F32)


def attention_forward_kernel(chunk, block, start_tab, start_ref, q_ref, *refs):
    n_kv = chunk + 1
    k_refs, v_refs = refs[:n_kv], refs[n_kv:2 * n_kv]
    o_ref, lse_ref, k_all, v_t, row_max, row_sum, acc = refs[2 * n_kv:]
    length, dim = q_ref.shape
    scale2 = dim ** -0.5 * LOG2_E
    for i in range(n_kv):
        k_all[i * length:(i + 1) * length, :] = k_refs[i][...]
        v_t[:, i * length:(i + 1) * length] = v_refs[i][...].T
    for sub in range(length // block):
        rows = slice(sub * block, (sub + 1) * block)
        q0 = chunk * length + sub * block
        q_t = q_ref[rows, :].T
        starts = start_ref[:, rows]
        last_start = start_tab[q0 + block - 1]
        row_max[...] = jnp.full(row_max.shape, MASKED, F32)
        row_sum[...] = jnp.zeros(row_sum.shape, F32)
        acc[...] = jnp.zeros(acc.shape, F32)

        def step(j, masked):
            k0 = pl.multiple_of(j * block, block)
            scores = dot32(k_all[pl.ds(k0, block), :], q_t, 1, 0)
            if masked:
                k_pos = k0 + lax.broadcasted_iota(jnp.int32, (block, block), 0)
                q_pos = q0 + lax.broadcasted_iota(jnp.int32, (block, block), 1)
                scores = jnp.where((k_pos <= q_pos) & (k_pos >= starts), scores, MASKED)
            old_max = row_max[...]
            new_max = jnp.maximum(old_max, jnp.max(scores, axis=0, keepdims=True))
            fade = jnp.exp2((old_max - new_max) * scale2)
            prob = jnp.exp2((scores - new_max) * scale2)
            row_max[...] = new_max
            row_sum[...] = row_sum[...] * fade + jnp.sum(prob, axis=0, keepdims=True)
            acc[...] = acc[...] * fade + dot32(v_t[:, pl.ds(k0, block)], prob.astype(BF16), 1, 0)

        def body(j, carry):
            needs_mask = (j * block + block - 1 > q0) | (j * block < last_start)
            pl.when(needs_mask)(lambda: step(j, True))
            pl.when(jnp.logical_not(needs_mask))(lambda: step(j, False))
            return carry

        lax.fori_loop(start_tab[q0] // block, q0 // block + 1, body, 0)
        o_ref[rows, :] = (acc[...] / row_sum[...]).T.astype(BF16)
        lse_ref[0, :, rows] = row_max[...] * scale2 + jnp.log2(row_sum[...])


def attention_forward(chunk, block, n_heads, start, qkv_chunks):
    length, width = qkv_chunks[0].shape
    dim = width // (3 * n_heads)
    n_kv = chunk + 1
    spec = lambda part: pl.BlockSpec((length, dim), lambda n, tab: (0, 3 * n + part))
    pairs = n_heads * length * (chunk * length + length // 2)
    return pl.pallas_call(
        functools.partial(attention_forward_kernel, chunk, block),
        grid_spec=pltpu.PrefetchScalarGridSpec(
            num_scalar_prefetch=1,
            grid=(n_heads,),
            in_specs=[pl.BlockSpec((1, length), lambda n, tab: (0, chunk)), spec(0)] + [spec(1)] * n_kv + [spec(2)] * n_kv,
            out_specs=[
                pl.BlockSpec((length, dim), lambda n, tab: (0, n)),
                pl.BlockSpec((1, 1, length), lambda n, tab: (n, 0, 0)),
            ],
            scratch_shapes=[
                pltpu.VMEM((n_kv * length, dim), BF16),
                pltpu.VMEM((dim, n_kv * length), BF16),
                pltpu.VMEM((1, block), F32),
                pltpu.VMEM((1, block), F32),
                pltpu.VMEM((dim, block), F32),
            ],
        ),
        out_shape=[
            jax.ShapeDtypeStruct((length, n_heads * dim), BF16),
            jax.ShapeDtypeStruct((n_heads, 1, length), F32),
        ],
        cost_estimate=pl.CostEstimate(flops=8 * pairs * dim, bytes_accessed=8 * length * width, transcendentals=pairs),
        name=f'attn_fwd_{chunk}',
    )(start, start.reshape(1, -1), qkv_chunks[chunk], *qkv_chunks[:n_kv], *qkv_chunks[:n_kv])


def attention_backward_kernel(chunk, last, block, start_tab, start_ref, lse_ref, q_ref, do_ref, o_ref, *refs):
    n_kv = chunk + 1
    k_refs, v_refs, refs = refs[:n_kv], refs[n_kv:2 * n_kv], refs[2 * n_kv:]
    if not last:
        dk_in, dv_in, refs = refs[0], refs[1], refs[2:]
    dqkv_ref, refs = refs[0], refs[1:]
    if chunk:
        dk_out, dv_out, refs = refs[0], refs[1], refs[2:]
    k_all, v_all, k_t, dk_sum, dv_sum, dq_t = refs
    length, dim = q_ref.shape
    scale = dim ** -0.5
    scale2 = scale * LOG2_E
    for i in range(n_kv):
        rows = slice(i * length, (i + 1) * length)
        k_all[rows, :] = k_refs[i][...]
        v_all[rows, :] = v_refs[i][...]
        k_t[:, rows] = k_refs[i][...].T
    if last:
        dk_sum[...] = jnp.zeros(dk_sum.shape, F32)
        dv_sum[...] = jnp.zeros(dv_sum.shape, F32)
    else:
        dk_sum[...] = dk_in[...]
        dv_sum[...] = dv_in[...]
    for sub in range(length // block):
        rows = slice(sub * block, (sub + 1) * block)
        q0 = chunk * length + sub * block
        q_blk = q_ref[rows, :]
        do_blk = do_ref[rows, :]
        q_t = q_blk.T
        do_t = do_blk.T
        delta = jnp.sum((do_blk.astype(F32) * o_ref[rows, :].astype(F32)).T, axis=0, keepdims=True)
        lse = lse_ref[0, :, rows]
        starts = start_ref[:, rows]
        last_start = start_tab[q0 + block - 1]
        dq_t[...] = jnp.zeros(dq_t.shape, F32)

        def step(j, masked):
            k0 = pl.multiple_of(j * block, block)
            keys = pl.ds(k0, block)
            scores = dot32(k_all[keys, :], q_t, 1, 0)
            prob = jnp.exp2(scores * scale2 - lse)
            if masked:
                k_pos = k0 + lax.broadcasted_iota(jnp.int32, (block, block), 0)
                q_pos = q0 + lax.broadcasted_iota(jnp.int32, (block, block), 1)
                prob = jnp.where((k_pos <= q_pos) & (k_pos >= starts), prob, 0.0)
            d_prob = dot32(v_all[keys, :], do_t, 1, 0)
            d_score = (prob * (d_prob - delta)).astype(BF16)
            dv_sum[keys, :] += dot32(prob.astype(BF16), do_blk, 1, 0)
            dk_sum[keys, :] += dot32(d_score, q_blk, 1, 0)
            dq_t[...] += dot32(k_t[:, keys], d_score, 1, 0)

        def body(j, carry):
            needs_mask = (j * block + block - 1 > q0) | (j * block < last_start)
            pl.when(needs_mask)(lambda: step(j, True))
            pl.when(jnp.logical_not(needs_mask))(lambda: step(j, False))
            return carry

        lax.fori_loop(start_tab[q0] // block, q0 // block + 1, body, 0)
        dqkv_ref[rows, :dim] = (dq_t[...] * scale).T.astype(BF16)
    own = slice(chunk * length, n_kv * length)
    dqkv_ref[:, dim:2 * dim] = (dk_sum[own, :] * scale).astype(BF16)
    dqkv_ref[:, 2 * dim:] = dv_sum[own, :].astype(BF16)
    if chunk:
        dk_out[...] = dk_sum[:chunk * length, :]
        dv_out[...] = dv_sum[:chunk * length, :]


def attention_backward(chunk, last, block, n_heads, start, qkv_chunks, lse, d_attn, attn_out, sums):
    length, width = qkv_chunks[0].shape
    dim = width // (3 * n_heads)
    n_kv = chunk + 1
    spec = lambda part: pl.BlockSpec((length, dim), lambda n, tab: (0, 3 * n + part))
    head = lambda rows: pl.BlockSpec((rows, dim), lambda n, tab: (0, n))
    pairs = n_heads * length * (chunk * length + length // 2)
    out_specs = [pl.BlockSpec((length, 3 * dim), lambda n, tab: (0, n))]
    out_shape = [jax.ShapeDtypeStruct((length, width), BF16)]
    if chunk:
        out_specs += [head(chunk * length)] * 2
        out_shape += [jax.ShapeDtypeStruct((chunk * length, n_heads * dim), F32)] * 2
    outs = pl.pallas_call(
        functools.partial(attention_backward_kernel, chunk, last, block),
        grid_spec=pltpu.PrefetchScalarGridSpec(
            num_scalar_prefetch=1,
            grid=(n_heads,),
            in_specs=[
                pl.BlockSpec((1, length), lambda n, tab: (0, chunk)),
                pl.BlockSpec((1, 1, length), lambda n, tab: (n, 0, 0)),
                spec(0), head(length), head(length),
            ] + [spec(1)] * n_kv + [spec(2)] * n_kv + ([] if last else [head(n_kv * length)] * 2),
            out_specs=out_specs,
            scratch_shapes=[
                pltpu.VMEM((n_kv * length, dim), BF16),
                pltpu.VMEM((n_kv * length, dim), BF16),
                pltpu.VMEM((dim, n_kv * length), BF16),
                pltpu.VMEM((n_kv * length, dim), F32),
                pltpu.VMEM((n_kv * length, dim), F32),
                pltpu.VMEM((dim, block), F32),
            ],
        ),
        out_shape=out_shape,
        cost_estimate=pl.CostEstimate(flops=20 * pairs * dim, bytes_accessed=12 * length * width, transcendentals=pairs),
        name=f'attn_bwd_{chunk}',
    )(start, start.reshape(1, -1), lse, qkv_chunks[chunk], d_attn, attn_out, *qkv_chunks[:n_kv], *qkv_chunks[:n_kv], *sums)
    return outs[0], tuple(outs[1:])


class Order:
    def __init__(self):
        self.token = None

    def after(self, *args):
        if self.token is None:
            return args
        *args, self.token = lax.optimization_barrier((*args, self.token))
        return args

    def done(self, value):
        self.token = value
        return value


def solution(mesh):
    n_dev = mesh.shape['model']

    def local_step(x_in, seg_ids, gain_one, w_qkv, w_out, gain_two, w_up, w_down, d_y):
        seq_len, width = x_in.shape[1:]
        n_heads, head_dim = w_out.shape[:2]
        n_chunks = 4
        length = seq_len // n_chunks
        part = length // n_dev
        block = min(512, length)
        x_in, d_y, seg = x_in[0], d_y[0], seg_ids[0]
        w_out = w_out.reshape(n_heads * head_dim, width)
        gain_one32, gain_two32 = gain_one.astype(F32), gain_two.astype(F32)
        me = lax.axis_index('model')
        chunks = range(n_chunks)
        order = Order()

        def chunk_of(array, c):
            return lax.slice_in_dim(array, c * length, (c + 1) * length, axis=0)

        def shard_of(array, c):
            return lax.dynamic_slice_in_dim(array, c * length + me * part, part, axis=0)

        def scatter(value):
            return lax.psum_scatter(value, 'model', scatter_dimension=0, tiled=True)

        def gather(value):
            return lax.all_gather(value, 'model', axis=0, tiled=True)

        def matmul(lhs, rhs, lhs_dim, rhs_dim, chunk=None):
            lhs, rhs = order.after(lhs, rhs)
            lhs = lhs if chunk is None else chunk_of(lhs, chunk)
            return order.done(dot32(lhs, rhs, lhs_dim, rhs_dim).astype(BF16))

        start = jnp.sum((seg[None, :] < seg[:, None]).astype(jnp.int32), axis=1)
        normed_one = order.done(layer_norm(x_in, gain_one))

        qkv, attn, lse = [], [], []
        sum_one, resid, full_two = {}, {}, {}
        d_gelu, gelu_out, d_up = {}, {}, {}
        sum_two, y_rows = {}, {}
        sum_norm_two, d_resid, d_resid_full, d_gain_two = {}, {}, {}, {}
        d_qkv, sum_norm_one, d_x_rows, d_gain_one = {}, {}, {}, {}
        sums = ()

        def attention_in(c):
            qkv.append(matmul(normed_one, w_qkv, 1, 0, c))
            attn_c, lse_c = attention_forward(c, block, n_heads, start, qkv)
            attn.append(order.done(attn_c))
            lse.append(lse_c)
            sum_one[c] = scatter(matmul(attn_c, w_out, 1, 0))

        def second_norm(c):
            (total,) = order.after(sum_one[c])
            resid[c] = (shard_of(x_in, c).astype(F32) + total.astype(F32)).astype(BF16)
            full_two[c] = gather(order.done(layer_norm(resid[c], gain_two)))

        def gelu_back(c):
            d_gelu[c] = matmul(d_y, w_down, 1, 1, c)

        def up(c):
            up_proj = matmul(full_two[c], w_up, 1, 0)
            gelu_c, gelu_pull = jax.vjp(gelu_tanh, up_proj)
            gelu_out[c], d_up[c] = lax.optimization_barrier((gelu_c, gelu_pull(d_gelu[c])[0]))
            order.done(d_up[c])

        def down(c):
            sum_two[c] = scatter(matmul(gelu_out[c], w_down, 1, 0))

        def finish_y(c):
            (total,) = order.after(sum_two[c])
            y_rows[c] = order.done((resid[c].astype(F32) + total.astype(F32)).astype(BF16))

        def norm_two_part(c):
            sum_norm_two[c] = scatter(matmul(d_up[c], w_up, 1, 1))

        def second_norm_back(c):
            (total,) = order.after(sum_norm_two[c])
            _, pull = jax.vjp(layer_norm, resid[c], gain_two32)
            d_rows, d_gain_two[c] = pull(total)
            d_resid[c] = order.done(shard_of(d_y, c) + d_rows)
            d_resid_full[c] = gather(d_resid[c])

        def attention_back(c):
            nonlocal sums
            d_attn = matmul(d_resid_full[c], w_out, 1, 1)
            d_qkv[c], sums = attention_backward(c, c == n_chunks - 1, block, n_heads, start, qkv, lse[c], d_attn, attn[c], sums)
            order.done(d_qkv[c])
            sum_norm_one[c] = scatter(matmul(d_qkv[c], w_qkv, 1, 1))

        def first_norm_back(c):
            (total,) = order.after(sum_norm_one[c])
            _, pull = jax.vjp(layer_norm, shard_of(x_in, c), gain_one32)
            d_rows, d_gain_one[c] = pull(total)
            d_x_rows[c] = order.done(d_resid[c] + d_rows)

        def weight_grad(lhs, rhs, which):
            total = None
            for c in which:
                l_c, r_c = order.after(lhs(c), rhs(c))
                r_c = r_c if r_c.shape[0] == length else chunk_of(r_c, c)
                term = dot32(l_c, r_c, 0, 0)
                total = order.done(term if total is None else total + term)
            return order.done(total.astype(BF16))

        def gather_all(rows):
            stacked = jnp.stack([rows[c] for c in chunks])
            return lax.all_gather(stacked, 'model', axis=1, tiled=True).reshape(seq_len, width)

        attention_in(0)
        attention_in(1)
        attention_in(2)
        second_norm(0)
        attention_in(3)
        second_norm(1)
        gelu_back(0)
        gelu_back(1)
        second_norm(2)
        gelu_back(2)
        gelu_back(3)
        second_norm(3)
        up(0)
        up(1)
        down(0)
        up(2)
        down(1)
        up(3)
        norm_two_part(3)
        norm_two_part(2)
        finish_y(0)
        norm_two_part(1)
        second_norm_back(3)
        norm_two_part(0)
        second_norm_back(2)
        finish_y(1)
        d_w_down = weight_grad(gelu_out.get, lambda c: d_y, chunks)
        second_norm_back(1)
        attention_back(3)
        second_norm_back(0)
        attention_back(2)
        down(2)
        attention_back(1)
        down(3)
        attention_back(0)
        first_norm_back(3)
        first_norm_back(2)
        d_w_up = weight_grad(full_two.get, d_up.get, chunks)
        finish_y(2)
        d_w_out = weight_grad(attn.__getitem__, d_resid_full.get, chunks)
        first_norm_back(1)
        finish_y(3)
        y_out = gather_all(y_rows)
        first_norm_back(0)
        d_x = gather_all(d_x_rows)
        d_qkv_all, normed_all = order.after(jnp.concatenate([d_qkv[c] for c in chunks], axis=0), normed_one)
        d_w_qkv = dot32(normed_all, d_qkv_all, 0, 0).astype(BF16)
        d_gains = lax.psum(jnp.stack([sum(d_gain_one[c] for c in chunks), sum(d_gain_two[c] for c in chunks)]), 'model').astype(BF16)
        return y_out[None], d_x[None], d_w_qkv, d_w_out.reshape(n_heads, head_dim, width), d_w_up, d_w_down, d_gains[0], d_gains[1]

    in_specs = (P('data'), P('data'), P(), P(None, 'model'), P('model'), P(), P(None, 'model'), P('model'), P('data'))
    out_specs = (P('data'), P('data'), P('data', 'model'), P(('data', 'model')), P('data', 'model'), P(('data', 'model')), P('data'), P('data'))
    return jax.shard_map(local_step, mesh=mesh, in_specs=in_specs, out_specs=out_specs, check_vma=False)
```

```python
import functools

import jax
import jax.numpy as jnp
from jax import lax
from jax.experimental import pallas as pl
from jax.experimental.pallas import tpu as pltpu
from jax.sharding import PartitionSpec as P

LN_EPS = 1e-5
LOG2_E = 1.4426950408889634
MASKED = -1e30
F32 = jnp.float32
BF16 = jnp.bfloat16


def norm_parts(rows):
    centered = rows - jnp.mean(rows, axis=-1, keepdims=True)
    rstd = lax.rsqrt(jnp.mean(centered * centered, axis=-1, keepdims=True) + LN_EPS)
    return centered * rstd, rstd


def norm_kernel(x_ref, gain_ref, out_ref):
    out_ref[...] = (norm_parts(x_ref[...].astype(F32))[0] * gain_ref[...].astype(F32)).astype(BF16)


def norm_all(x_in, gain, rows=256):
    seq_len, width = x_in.shape
    return pl.pallas_call(
        norm_kernel,
        grid=(seq_len // rows,),
        in_specs=[pl.BlockSpec((rows, width), lambda i: (i, 0)), pl.BlockSpec((1, width), lambda i: (0, 0))],
        out_specs=pl.BlockSpec((rows, width), lambda i: (i, 0)),
        out_shape=jax.ShapeDtypeStruct(x_in.shape, BF16),
        cost_estimate=pl.CostEstimate(flops=10 * seq_len * width, bytes_accessed=4 * seq_len * width, transcendentals=0),
        name='norm_all',
    )(x_in, gain.reshape(1, -1))


def add_norm_kernel(where_ref, x_ref, sum_ref, gain_ref, resid_ref, out_ref):
    resid = (x_ref[...].astype(F32) + sum_ref[...].astype(F32)).astype(BF16)
    resid_ref[...] = resid
    out_ref[...] = (norm_parts(resid.astype(F32))[0] * gain_ref[...].astype(F32)).astype(BF16)


def add_norm(where, x_in, total, gain, rows=32):
    n_rows, width = total.shape
    steps = n_rows // rows
    own = pl.BlockSpec((rows, width), lambda i, w: (i, 0))
    return pl.pallas_call(
        add_norm_kernel,
        grid_spec=pltpu.PrefetchScalarGridSpec(
            num_scalar_prefetch=1,
            grid=(steps,),
            in_specs=[pl.BlockSpec((rows, width), lambda i, w: (w[0] * steps + i, 0)), own, pl.BlockSpec((1, width), lambda i, w: (0, 0))],
            out_specs=[own, own],
        ),
        out_shape=[jax.ShapeDtypeStruct(total.shape, BF16)] * 2,
        cost_estimate=pl.CostEstimate(flops=20 * n_rows * width, bytes_accessed=8 * n_rows * width, transcendentals=0),
        name='add_norm',
    )(where, x_in, total, gain.reshape(1, -1))


def norm_back_kernel(where_ref, x_ref, base_ref, d_ref, gain_ref, out_ref, d_gain_ref):
    normed, rstd = norm_parts(x_ref[...].astype(F32))
    d_out = d_ref[...].astype(F32)
    d_normed = d_out * gain_ref[...].astype(F32)
    inner = jnp.mean(d_normed * normed, axis=-1, keepdims=True)
    d_rows = (rstd * (d_normed - jnp.mean(d_normed, axis=-1, keepdims=True) - normed * inner)).astype(BF16)
    out_ref[...] = (base_ref[...].astype(F32) + d_rows.astype(F32)).astype(BF16)

    @pl.when(pl.program_id(0) == 0)
    def _():
        d_gain_ref[...] = jnp.zeros(d_gain_ref.shape, F32)

    d_gain_ref[...] += jnp.sum(d_out * normed, axis=0, keepdims=True)


def norm_back(where, x_rows, base_rows, d_rows, gain, rows=32):
    n_rows, width = d_rows.shape
    steps = n_rows // rows
    own = pl.BlockSpec((rows, width), lambda i, w: (i, 0))
    spec = lambda a: own if a.shape[0] == n_rows else pl.BlockSpec((rows, width), lambda i, w: (w[0] * steps + i, 0))
    flat = pl.BlockSpec((1, width), lambda i, w: (0, 0))
    return pl.pallas_call(
        norm_back_kernel,
        grid_spec=pltpu.PrefetchScalarGridSpec(
            num_scalar_prefetch=1,
            grid=(steps,),
            in_specs=[spec(x_rows), spec(base_rows), own, flat],
            out_specs=[own, flat],
        ),
        out_shape=[jax.ShapeDtypeStruct(d_rows.shape, BF16), jax.ShapeDtypeStruct((1, width), F32)],
        cost_estimate=pl.CostEstimate(flops=30 * n_rows * width, bytes_accessed=8 * n_rows * width, transcendentals=0),
        name='norm_back',
    )(where, x_rows, base_rows, d_rows, gain.reshape(1, -1))


def copy_kernel(src_ref, *refs):
    refs[-1][...] = src_ref[...]


def place(src, seq_len, at, into=None, rows=256):
    n_rows, width = src.shape
    shift = at // rows
    more = [] if into is None else [into]
    return pl.pallas_call(
        copy_kernel,
        grid=(n_rows // rows,),
        in_specs=[pl.BlockSpec((rows, width), lambda i: (i, 0))] + [pl.BlockSpec(memory_space=pl.ANY)] * len(more),
        out_specs=pl.BlockSpec((rows, width), lambda i: (i + shift, 0)),
        out_shape=jax.ShapeDtypeStruct((seq_len, width), src.dtype),
        input_output_aliases={} if into is None else {1: 0},
        cost_estimate=pl.CostEstimate(flops=n_rows * width, bytes_accessed=4 * n_rows * width, transcendentals=0),
        name='place',
    )(src, *more)


def gelu_tanh(up_proj):
    return jax.nn.gelu(up_proj.astype(F32), approximate=True).astype(BF16)


def dot32(lhs, rhs, lhs_dim, rhs_dim):
    return lax.dot_general(lhs, rhs, (((lhs_dim,), (rhs_dim,)), ((), ())), preferred_element_type=F32)


def attention_forward_kernel(chunk, block, start_tab, start_ref, q_ref, *refs):
    n_kv = chunk + 1
    k_refs, v_refs = refs[:n_kv], refs[n_kv:2 * n_kv]
    o_ref, lse_ref, k_all, v_t, row_max, row_sum, acc = refs[2 * n_kv:]
    length, dim = q_ref.shape
    scale2 = dim ** -0.5 * LOG2_E
    for i in range(n_kv):
        k_all[i * length:(i + 1) * length, :] = k_refs[i][...]
        v_t[:, i * length:(i + 1) * length] = v_refs[i][...].T
    for sub in range(length // block):
        rows = slice(sub * block, (sub + 1) * block)
        q0 = chunk * length + sub * block
        q_t = q_ref[rows, :].T
        starts = start_ref[:, rows]
        last_start = start_tab[q0 + block - 1]
        row_max[...] = jnp.full(row_max.shape, MASKED, F32)
        row_sum[...] = jnp.zeros(row_sum.shape, F32)
        acc[...] = jnp.zeros(acc.shape, F32)

        def step(j, masked):
            k0 = pl.multiple_of(j * block, block)
            scores = dot32(k_all[pl.ds(k0, block), :], q_t, 1, 0)
            if masked:
                k_pos = k0 + lax.broadcasted_iota(jnp.int32, (block, block), 0)
                q_pos = q0 + lax.broadcasted_iota(jnp.int32, (block, block), 1)
                scores = jnp.where((k_pos <= q_pos) & (k_pos >= starts), scores, MASKED)
            old_max = row_max[...]
            new_max = jnp.maximum(old_max, jnp.max(scores, axis=0, keepdims=True))
            fade = jnp.exp2((old_max - new_max) * scale2)
            prob = jnp.exp2((scores - new_max) * scale2)
            row_max[...] = new_max
            row_sum[...] = row_sum[...] * fade + jnp.sum(prob, axis=0, keepdims=True)
            acc[...] = acc[...] * fade + dot32(v_t[:, pl.ds(k0, block)], prob.astype(BF16), 1, 0)

        def body(j, carry):
            needs_mask = (j * block + block - 1 > q0) | (j * block < last_start)
            pl.when(needs_mask)(lambda: step(j, True))
            pl.when(jnp.logical_not(needs_mask))(lambda: step(j, False))
            return carry

        lax.fori_loop(start_tab[q0] // block, q0 // block + 1, body, 0)
        o_ref[rows, :] = (acc[...] / row_sum[...]).T.astype(BF16)
        lse_ref[0, :, rows] = row_max[...] * scale2 + jnp.log2(row_sum[...])


def attention_forward(chunk, block, n_heads, start, qkv_chunks):
    length, width = qkv_chunks[0].shape
    dim = width // (3 * n_heads)
    n_kv = chunk + 1
    spec = lambda part: pl.BlockSpec((length, dim), lambda n, tab: (0, 3 * n + part))
    pairs = n_heads * length * (chunk * length + length // 2)
    return pl.pallas_call(
        functools.partial(attention_forward_kernel, chunk, block),
        grid_spec=pltpu.PrefetchScalarGridSpec(
            num_scalar_prefetch=1,
            grid=(n_heads,),
            in_specs=[pl.BlockSpec((1, length), lambda n, tab: (0, chunk)), spec(0)] + [spec(1)] * n_kv + [spec(2)] * n_kv,
            out_specs=[
                pl.BlockSpec((length, dim), lambda n, tab: (0, n)),
                pl.BlockSpec((1, 1, length), lambda n, tab: (n, 0, 0)),
            ],
            scratch_shapes=[
                pltpu.VMEM((n_kv * length, dim), BF16),
                pltpu.VMEM((dim, n_kv * length), BF16),
                pltpu.VMEM((1, block), F32),
                pltpu.VMEM((1, block), F32),
                pltpu.VMEM((dim, block), F32),
            ],
        ),
        out_shape=[
            jax.ShapeDtypeStruct((length, n_heads * dim), BF16),
            jax.ShapeDtypeStruct((n_heads, 1, length), F32),
        ],
        cost_estimate=pl.CostEstimate(flops=8 * pairs * dim, bytes_accessed=8 * length * width, transcendentals=pairs),
        name=f'attn_fwd_{chunk}',
    )(start, start.reshape(1, -1), qkv_chunks[chunk], *qkv_chunks[:n_kv], *qkv_chunks[:n_kv])


def attention_backward_kernel(chunk, last, block, start_tab, start_ref, lse_ref, q_ref, do_ref, o_ref, *refs):
    n_kv = chunk + 1
    k_refs, v_refs, refs = refs[:n_kv], refs[n_kv:2 * n_kv], refs[2 * n_kv:]
    if not last:
        dk_in, dv_in, refs = refs[0], refs[1], refs[2:]
    dqkv_ref, refs = refs[0], refs[1:]
    if chunk:
        dk_out, dv_out, refs = refs[0], refs[1], refs[2:]
    k_all, v_all, k_t, dk_sum, dv_sum, dq_t = refs
    length, dim = q_ref.shape
    scale = dim ** -0.5
    scale2 = scale * LOG2_E
    for i in range(n_kv):
        rows = slice(i * length, (i + 1) * length)
        k_all[rows, :] = k_refs[i][...]
        v_all[rows, :] = v_refs[i][...]
        k_t[:, rows] = k_refs[i][...].T
    if last:
        dk_sum[...] = jnp.zeros(dk_sum.shape, F32)
        dv_sum[...] = jnp.zeros(dv_sum.shape, F32)
    else:
        dk_sum[...] = dk_in[...]
        dv_sum[...] = dv_in[...]
    for sub in range(length // block):
        rows = slice(sub * block, (sub + 1) * block)
        q0 = chunk * length + sub * block
        q_blk = q_ref[rows, :]
        do_blk = do_ref[rows, :]
        q_t = q_blk.T
        do_t = do_blk.T
        delta = jnp.sum((do_blk.astype(F32) * o_ref[rows, :].astype(F32)).T, axis=0, keepdims=True)
        lse = lse_ref[0, :, rows]
        starts = start_ref[:, rows]
        last_start = start_tab[q0 + block - 1]
        dq_t[...] = jnp.zeros(dq_t.shape, F32)

        def step(j, masked):
            k0 = pl.multiple_of(j * block, block)
            keys = pl.ds(k0, block)
            scores = dot32(k_all[keys, :], q_t, 1, 0)
            prob = jnp.exp2(scores * scale2 - lse)
            if masked:
                k_pos = k0 + lax.broadcasted_iota(jnp.int32, (block, block), 0)
                q_pos = q0 + lax.broadcasted_iota(jnp.int32, (block, block), 1)
                prob = jnp.where((k_pos <= q_pos) & (k_pos >= starts), prob, 0.0)
            d_prob = dot32(v_all[keys, :], do_t, 1, 0)
            d_score = (prob * (d_prob - delta)).astype(BF16)
            dv_sum[keys, :] += dot32(prob.astype(BF16), do_blk, 1, 0)
            dk_sum[keys, :] += dot32(d_score, q_blk, 1, 0)
            dq_t[...] += dot32(k_t[:, keys], d_score, 1, 0)

        def body(j, carry):
            needs_mask = (j * block + block - 1 > q0) | (j * block < last_start)
            pl.when(needs_mask)(lambda: step(j, True))
            pl.when(jnp.logical_not(needs_mask))(lambda: step(j, False))
            return carry

        lax.fori_loop(start_tab[q0] // block, q0 // block + 1, body, 0)
        dqkv_ref[rows, :dim] = (dq_t[...] * scale).T.astype(BF16)
    own = slice(chunk * length, n_kv * length)
    dqkv_ref[:, dim:2 * dim] = (dk_sum[own, :] * scale).astype(BF16)
    dqkv_ref[:, 2 * dim:] = dv_sum[own, :].astype(BF16)
    if chunk:
        dk_out[...] = dk_sum[:chunk * length, :]
        dv_out[...] = dv_sum[:chunk * length, :]


def attention_backward(chunk, last, block, n_heads, start, qkv_chunks, lse, d_attn, attn_out, sums):
    length, width = qkv_chunks[0].shape
    dim = width // (3 * n_heads)
    n_kv = chunk + 1
    spec = lambda part: pl.BlockSpec((length, dim), lambda n, tab: (0, 3 * n + part))
    head = lambda rows: pl.BlockSpec((rows, dim), lambda n, tab: (0, n))
    pairs = n_heads * length * (chunk * length + length // 2)
    out_specs = [pl.BlockSpec((length, 3 * dim), lambda n, tab: (0, n))]
    out_shape = [jax.ShapeDtypeStruct((length, width), BF16)]
    if chunk:
        out_specs += [head(chunk * length)] * 2
        out_shape += [jax.ShapeDtypeStruct((chunk * length, n_heads * dim), F32)] * 2
    outs = pl.pallas_call(
        functools.partial(attention_backward_kernel, chunk, last, block),
        grid_spec=pltpu.PrefetchScalarGridSpec(
            num_scalar_prefetch=1,
            grid=(n_heads,),
            in_specs=[
                pl.BlockSpec((1, length), lambda n, tab: (0, chunk)),
                pl.BlockSpec((1, 1, length), lambda n, tab: (n, 0, 0)),
                spec(0), head(length), head(length),
            ] + [spec(1)] * n_kv + [spec(2)] * n_kv + ([] if last else [head(n_kv * length)] * 2),
            out_specs=out_specs,
            scratch_shapes=[
                pltpu.VMEM((n_kv * length, dim), BF16),
                pltpu.VMEM((n_kv * length, dim), BF16),
                pltpu.VMEM((dim, n_kv * length), BF16),
                pltpu.VMEM((n_kv * length, dim), F32),
                pltpu.VMEM((n_kv * length, dim), F32),
                pltpu.VMEM((dim, block), F32),
            ],
        ),
        out_shape=out_shape,
        cost_estimate=pl.CostEstimate(flops=20 * pairs * dim, bytes_accessed=12 * length * width, transcendentals=pairs),
        name=f'attn_bwd_{chunk}',
    )(start, start.reshape(1, -1), lse, qkv_chunks[chunk], d_attn, attn_out, *qkv_chunks[:n_kv], *qkv_chunks[:n_kv], *sums)
    return outs[0], tuple(outs[1:])


class Order:
    def __init__(self):
        self.token = None

    def after(self, *args):
        if self.token is None:
            return args
        *args, self.token = lax.optimization_barrier((*args, self.token))
        return args

    def done(self, value):
        self.token = value
        return value


def solution(mesh):
    n_dev = mesh.shape['model']

    def local_step(x_in, seg_ids, gain_one, w_qkv, w_out, gain_two, w_up, w_down, d_y):
        seq_len, width = x_in.shape[1:]
        n_heads, head_dim = w_out.shape[:2]
        n_chunks = 4
        length = seq_len // n_chunks
        part = length // n_dev
        block = min(512, length)
        x_in, d_y, seg = x_in[0], d_y[0], seg_ids[0]
        w_out = w_out.reshape(n_heads * head_dim, width)
        me = lax.axis_index('model')
        core = me % 2
        n_chips = n_dev // 2
        chunks = range(n_chunks)
        order = Order()
        swap = [(i, i ^ 1) for i in range(n_dev)]
        same_core = [[2 * i + k for i in range(n_chips)] for k in range(2)]

        def chunk_of(array, c):
            return lax.slice_in_dim(array, c * length, (c + 1) * length, axis=0)

        def where(c):
            return (c * n_dev + me).astype(jnp.int32).reshape(1)

        def matmul(lhs, rhs, lhs_dim, rhs_dim, chunk=None):
            lhs, rhs = order.after(lhs, rhs)
            lhs = lhs if chunk is None else chunk_of(lhs, chunk)
            return order.done(dot32(lhs, rhs, lhs_dim, rhs_dim).astype(BF16))

        def rows_of_core(array, which):
            tiles = array.reshape(n_chips, 2, part, array.shape[-1])
            return lax.dynamic_index_in_dim(tiles, which, axis=1, keepdims=False).reshape(n_chips * part, -1)

        def send_half(lhs, rhs, rhs_dim):
            lhs, rhs = order.after(lhs, rhs)
            away = order.done(dot32(rows_of_core(lhs, 1 - core), rhs, 1, rhs_dim).astype(BF16))
            return lax.ppermute(away, 'model', swap)

        def sum_half(lhs, rhs, rhs_dim, arrived):
            lhs, rhs, arrived = order.after(lhs, rhs, arrived)
            both = order.done((dot32(rows_of_core(lhs, core), rhs, 1, rhs_dim) + arrived.astype(F32)).astype(BF16))
            return lax.psum_scatter(both, 'model', scatter_dimension=0, axis_index_groups=same_core, tiled=True)

        start = jnp.sum((seg[None, :] < seg[:, None]).astype(jnp.int32), axis=1)
        normed_one = order.done(norm_all(x_in, gain_one))

        qkv, attn, lse = [], [], []
        sent, total = {}, {}
        resid, normed_two, full_two, d_gelu, gelu_out, d_up, y_rows = {}, {}, {}, {}, {}, {}, {}
        d_resid, d_resid_full, d_gain_two, d_qkv, d_x_rows, d_gain_one = {}, {}, {}, {}, {}, {}
        sums = ()

        def qkv_in(c):
            qkv.append(matmul(normed_one, w_qkv, 1, 0, c))

        def attention_in(c):
            chunk_qkv = [*qkv[:c], order.after(qkv[c])[0]]
            attn_c, lse_c = attention_forward(c, block, n_heads, start, chunk_qkv)
            attn.append(order.done(attn_c))
            lse.append(lse_c)
            sent['one', c] = send_half(attn_c, w_out, 0)

        def out_proj(c):
            total['one', c] = sum_half(attn[c], w_out, 0, sent['one', c])

        def second_norm(c):
            (summed,) = order.after(total['one', c])
            resid[c], normed_two[c] = add_norm(where(c), x_in, summed, gain_two)
            order.done(normed_two[c])

        def gelu_back(c):
            d_gelu[c] = matmul(d_y, w_down, 1, 1, c)

        def up(c):
            up_proj = matmul(*full_two[c][:1], w_up, 1, 0, full_two[c][1])
            gelu_c, gelu_pull = jax.vjp(gelu_tanh, up_proj)
            gelu_out[c], d_up[c] = lax.optimization_barrier((gelu_c, gelu_pull(d_gelu[c])[0]))
            order.done(d_up[c])

        def down_send(c):
            sent['two', c] = send_half(gelu_out[c], w_down, 0)

        def down(c):
            total['two', c] = sum_half(gelu_out[c], w_down, 0, sent['two', c])

        def finish_y(c):
            (summed,) = order.after(total['two', c])
            y_rows[c] = order.done((resid[c].astype(F32) + summed.astype(F32)).astype(BF16))

        def norm_two_send(c):
            sent['norm_two', c] = send_half(d_up[c], w_up, 1)

        def norm_two(c):
            total['norm_two', c] = sum_half(d_up[c], w_up, 1, sent['norm_two', c])

        def second_norm_back(c):
            (summed,) = order.after(total['norm_two', c])
            d_resid[c], d_gain_two[c] = norm_back(where(c), resid[c], d_y, summed, gain_two)
            order.done(d_resid[c])

        d_attn = {}

        def attention_grad(c):
            d_attn[c] = matmul(d_resid_full[c][0], w_out, 1, 1, d_resid_full[c][1])

        def attention_back(c):
            nonlocal sums
            (d_out,) = order.after(d_attn[c])
            d_qkv[c], sums = attention_backward(c, c == n_chunks - 1, block, n_heads, start, qkv, lse[c], d_out, attn[c], sums)
            order.done(d_qkv[c])
            sent['norm_one', c] = send_half(d_qkv[c], w_qkv, 1)

        def norm_one(c):
            total['norm_one', c] = sum_half(d_qkv[c], w_qkv, 1, sent['norm_one', c])

        def first_norm_back(c):
            (summed,) = order.after(total['norm_one', c])
            d_x_rows[c], d_gain_one[c] = norm_back(where(c), x_in, d_resid[c], summed, gain_one)
            order.done(d_x_rows[c])

        def joined(parts, which=chunks):
            if len(which) == 1:
                return parts[which[0]]
            return order.done(jnp.concatenate(order.after(*(parts[c] for c in which)), axis=0))

        def weight_grad(*pairs):
            summed = None
            for lhs, rhs in pairs:
                term = dot32(*order.after(lhs, rhs), 0, 0)
                summed = order.done(term if summed is None else summed + term)
            return order.done(summed.astype(BF16))

        def gather(rows, which):
            if len(which) == 1:
                return lax.all_gather(rows[which[0]], 'model', axis=0, tiled=True)
            stacked = jnp.stack([rows[c] for c in which])
            return lax.all_gather(stacked, 'model', axis=1, tiled=True).reshape(len(which) * length, width)

        def share(rows, full, which):
            array = gather(rows, which)
            for i, c in enumerate(which):
                full[c] = (array, i)
            return array

        qkv_in(0)
        attention_in(0)
        out_proj(0)
        qkv_in(1)
        attention_in(1)
        qkv_in(2)
        out_proj(1)
        second_norm(0)
        two_0 = share(normed_two, full_two, [0])
        attention_in(2)
        qkv_in(3)
        out_proj(2)
        second_norm(1)
        two_1 = share(normed_two, full_two, [1])
        attention_in(3)
        gelu_back(0)
        out_proj(3)
        up(0)
        gelu_back(1)
        second_norm(2)
        down_send(0)
        up(1)
        second_norm(3)
        two_23 = share(normed_two, full_two, [2, 3])
        down(0)
        down_send(1)
        gelu_back(2)
        down(1)
        gelu_back(3)
        up(2)
        down_send(2)
        up(3)
        down(2)
        norm_two_send(3)
        norm_two_send(2)
        norm_two(3)
        norm_two_send(1)
        norm_two(2)
        norm_two_send(0)
        finish_y(0)
        gelu_all = joined(gelu_out)
        finish_y(1)
        finish_y(2)
        second_norm_back(3)
        second_norm_back(2)
        resid_23 = share(d_resid, d_resid_full, [2, 3])
        norm_two(1)
        norm_two(0)
        d_w_down = weight_grad((gelu_all, d_y))
        attention_grad(3)
        attention_back(3)
        second_norm_back(1)
        second_norm_back(0)
        resid_01 = share(d_resid, d_resid_full, [0, 1])
        attention_grad(2)
        norm_one(3)
        attention_back(2)
        down_send(3)
        norm_one(2)
        attention_grad(1)
        down(3)
        attention_back(1)
        attention_grad(0)
        norm_one(1)
        attention_back(0)
        d_up_23 = joined(d_up, [2, 3])
        norm_one(0)
        y_early = gather(y_rows, [0, 1, 2])
        first_norm_back(3)
        first_norm_back(2)
        d_w_out = weight_grad((joined(attn, [2, 3]), resid_23), (joined(attn, [0, 1]), resid_01))
        first_norm_back(1)
        d_x_late = gather(d_x_rows, [1, 2, 3])
        d_w_qkv = weight_grad((normed_one, joined(d_qkv)))
        first_norm_back(0)
        d_x_first = gather(d_x_rows, [0])
        finish_y(3)
        y_late = gather(y_rows, [3])
        gain_sums = order.done(jnp.concatenate(order.after(sum(d_gain_one[c] for c in chunks), sum(d_gain_two[c] for c in chunks))))
        d_gains = order.done(lax.psum(gain_sums, 'model').astype(BF16))
        d_w_up = weight_grad((two_0, d_up[0]), (two_1, d_up[1]), (two_23, d_up_23))
        y_out = order.done(place(order.after(y_early)[0], seq_len, 0))
        d_x = order.done(place(order.after(d_x_late)[0], seq_len, length))
        d_x = order.done(place(order.after(d_x_first)[0], seq_len, 0, d_x))
        y_out = place(order.after(y_late)[0], seq_len, 3 * length, y_out)
        return y_out[None], d_x[None], d_w_qkv, d_w_out.reshape(n_heads, head_dim, width), d_w_up, d_w_down, d_gains[0], d_gains[1]

    in_specs = (P('data'), P('data'), P(), P(None, 'model'), P('model'), P(), P(None, 'model'), P('model'), P('data'))
    out_specs = (P('data'), P('data'), P('data', 'model'), P(('data', 'model')), P('data', 'model'), P(('data', 'model')), P('data'), P('data'))
    return jax.shard_map(local_step, mesh=mesh, in_specs=in_specs, out_specs=out_specs, check_vma=False)
```

```python
import functools

import jax
import jax.numpy as jnp
from jax import lax
from jax.experimental import pallas as pl
from jax.experimental.pallas import tpu as pltpu
from jax.sharding import PartitionSpec as P

LN_EPS = 1e-5
LOG2_E = 1.4426950408889634
MASKED = -1e30
F32 = jnp.float32
BF16 = jnp.bfloat16


def norm_parts(rows):
    centered = rows - jnp.mean(rows, axis=-1, keepdims=True)
    rstd = lax.rsqrt(jnp.mean(centered * centered, axis=-1, keepdims=True) + LN_EPS)
    return centered * rstd, rstd


def norm_kernel(x_ref, gain_ref, *refs):
    refs[-1][...] = (norm_parts(x_ref[...].astype(F32))[0] * gain_ref[...].astype(F32)).astype(BF16)


def norm_rows(x_in, gain, first, last, into=None, rows=256):
    seq_len, width = x_in.shape
    shift = first // rows
    block = pl.BlockSpec((rows, width), lambda i: (i + shift, 0))
    more = [] if into is None else [into]
    return pl.pallas_call(
        norm_kernel,
        grid=((last - first) // rows,),
        in_specs=[block, pl.BlockSpec((1, width), lambda i: (0, 0))] + [pl.BlockSpec(memory_space=pl.ANY)] * len(more),
        out_specs=block,
        out_shape=jax.ShapeDtypeStruct(x_in.shape, BF16),
        input_output_aliases={} if into is None else {2: 0},
        cost_estimate=pl.CostEstimate(flops=10 * (last - first) * width, bytes_accessed=4 * (last - first) * width, transcendentals=0),
        name='norm_rows',
    )(x_in, gain.reshape(1, -1), *more)


def add_norm_kernel(where_ref, x_ref, sum_ref, gain_ref, resid_ref, out_ref):
    resid = (x_ref[...].astype(F32) + sum_ref[...].astype(F32)).astype(BF16)
    resid_ref[...] = resid
    out_ref[...] = (norm_parts(resid.astype(F32))[0] * gain_ref[...].astype(F32)).astype(BF16)


def add_norm(where, x_in, total, gain, rows=32):
    n_rows, width = total.shape
    steps = n_rows // rows
    own = pl.BlockSpec((rows, width), lambda i, w: (i, 0))
    return pl.pallas_call(
        add_norm_kernel,
        grid_spec=pltpu.PrefetchScalarGridSpec(
            num_scalar_prefetch=1,
            grid=(steps,),
            in_specs=[pl.BlockSpec((rows, width), lambda i, w: (w[0] * steps + i, 0)), own, pl.BlockSpec((1, width), lambda i, w: (0, 0))],
            out_specs=[own, own],
        ),
        out_shape=[jax.ShapeDtypeStruct(total.shape, BF16)] * 2,
        cost_estimate=pl.CostEstimate(flops=20 * n_rows * width, bytes_accessed=8 * n_rows * width, transcendentals=0),
        name='add_norm',
    )(where, x_in, total, gain.reshape(1, -1))


def norm_back_kernel(where_ref, x_ref, base_ref, d_ref, gain_ref, out_ref, d_gain_ref):
    normed, rstd = norm_parts(x_ref[...].astype(F32))
    d_out = d_ref[...].astype(F32)
    d_normed = d_out * gain_ref[...].astype(F32)
    inner = jnp.mean(d_normed * normed, axis=-1, keepdims=True)
    d_rows = (rstd * (d_normed - jnp.mean(d_normed, axis=-1, keepdims=True) - normed * inner)).astype(BF16)
    out_ref[...] = (base_ref[...].astype(F32) + d_rows.astype(F32)).astype(BF16)

    @pl.when(pl.program_id(0) == 0)
    def _():
        d_gain_ref[...] = jnp.zeros(d_gain_ref.shape, F32)

    d_gain_ref[...] += jnp.sum(d_out * normed, axis=0, keepdims=True)


def norm_back(where, x_rows, base_rows, d_rows, gain, rows=32):
    n_rows, width = d_rows.shape
    steps = n_rows // rows
    own = pl.BlockSpec((rows, width), lambda i, w: (i, 0))
    spec = lambda a: own if a.shape[0] == n_rows else pl.BlockSpec((rows, width), lambda i, w: (w[0] * steps + i, 0))
    flat = pl.BlockSpec((1, width), lambda i, w: (0, 0))
    return pl.pallas_call(
        norm_back_kernel,
        grid_spec=pltpu.PrefetchScalarGridSpec(
            num_scalar_prefetch=1,
            grid=(steps,),
            in_specs=[spec(x_rows), spec(base_rows), own, flat],
            out_specs=[own, flat],
        ),
        out_shape=[jax.ShapeDtypeStruct(d_rows.shape, BF16), jax.ShapeDtypeStruct((1, width), F32)],
        cost_estimate=pl.CostEstimate(flops=30 * n_rows * width, bytes_accessed=8 * n_rows * width, transcendentals=0),
        name='norm_back',
    )(where, x_rows, base_rows, d_rows, gain.reshape(1, -1))


def copy_kernel(src_ref, *refs):
    refs[-1][...] = src_ref[...]


def place(src, seq_len, at, into=None, rows=256):
    n_rows, width = src.shape
    shift = at // rows
    more = [] if into is None else [into]
    return pl.pallas_call(
        copy_kernel,
        grid=(n_rows // rows,),
        in_specs=[pl.BlockSpec((rows, width), lambda i: (i, 0))] + [pl.BlockSpec(memory_space=pl.ANY)] * len(more),
        out_specs=pl.BlockSpec((rows, width), lambda i: (i + shift, 0)),
        out_shape=jax.ShapeDtypeStruct((seq_len, width), src.dtype),
        input_output_aliases={} if into is None else {1: 0},
        cost_estimate=pl.CostEstimate(flops=n_rows * width, bytes_accessed=4 * n_rows * width, transcendentals=0),
        name='place',
    )(src, *more)


def gelu_tanh(up_proj):
    return jax.nn.gelu(up_proj.astype(F32), approximate=True).astype(BF16)


def dot32(lhs, rhs, lhs_dim, rhs_dim):
    return lax.dot_general(lhs, rhs, (((lhs_dim,), (rhs_dim,)), ((), ())), preferred_element_type=F32)


def attention_forward_kernel(chunk, block, start_tab, start_ref, q_ref, *refs):
    n_kv = chunk + 1
    k_refs, v_refs = refs[:n_kv], refs[n_kv:2 * n_kv]
    o_ref, lse_ref, k_all, v_t, row_max, row_sum, acc = refs[2 * n_kv:]
    length, dim = q_ref.shape
    scale2 = dim ** -0.5 * LOG2_E
    for i in range(n_kv):
        k_all[i * length:(i + 1) * length, :] = k_refs[i][...]
        v_t[:, i * length:(i + 1) * length] = v_refs[i][...].T
    for sub in range(length // block):
        rows = slice(sub * block, (sub + 1) * block)
        q0 = chunk * length + sub * block
        q_t = q_ref[rows, :].T
        starts = start_ref[:, rows]
        last_start = start_tab[q0 + block - 1]
        row_max[...] = jnp.full(row_max.shape, MASKED, F32)
        row_sum[...] = jnp.zeros(row_sum.shape, F32)
        acc[...] = jnp.zeros(acc.shape, F32)

        def step(j, masked):
            k0 = pl.multiple_of(j * block, block)
            scores = dot32(k_all[pl.ds(k0, block), :], q_t, 1, 0)
            if masked:
                k_pos = k0 + lax.broadcasted_iota(jnp.int32, (block, block), 0)
                q_pos = q0 + lax.broadcasted_iota(jnp.int32, (block, block), 1)
                scores = jnp.where((k_pos <= q_pos) & (k_pos >= starts), scores, MASKED)
            old_max = row_max[...]
            new_max = jnp.maximum(old_max, jnp.max(scores, axis=0, keepdims=True))
            fade = jnp.exp2((old_max - new_max) * scale2)
            prob = jnp.exp2((scores - new_max) * scale2)
            row_max[...] = new_max
            row_sum[...] = row_sum[...] * fade + jnp.sum(prob, axis=0, keepdims=True)
            acc[...] = acc[...] * fade + dot32(v_t[:, pl.ds(k0, block)], prob.astype(BF16), 1, 0)

        def body(j, carry):
            needs_mask = (j * block + block - 1 > q0) | (j * block < last_start)
            pl.when(needs_mask)(lambda: step(j, True))
            pl.when(jnp.logical_not(needs_mask))(lambda: step(j, False))
            return carry

        lax.fori_loop(start_tab[q0] // block, q0 // block + 1, body, 0)
        o_ref[rows, :] = (acc[...] / row_sum[...]).T.astype(BF16)
        lse_ref[0, :, rows] = row_max[...] * scale2 + jnp.log2(row_sum[...])


def attention_forward(chunk, block, n_heads, start, qkv_chunks):
    length, width = qkv_chunks[0].shape
    dim = width // (3 * n_heads)
    n_kv = chunk + 1
    spec = lambda part: pl.BlockSpec((length, dim), lambda n, tab: (0, 3 * n + part))
    pairs = n_heads * length * (chunk * length + length // 2)
    return pl.pallas_call(
        functools.partial(attention_forward_kernel, chunk, block),
        grid_spec=pltpu.PrefetchScalarGridSpec(
            num_scalar_prefetch=1,
            grid=(n_heads,),
            in_specs=[pl.BlockSpec((1, length), lambda n, tab: (0, chunk)), spec(0)] + [spec(1)] * n_kv + [spec(2)] * n_kv,
            out_specs=[
                pl.BlockSpec((length, dim), lambda n, tab: (0, n)),
                pl.BlockSpec((1, 1, length), lambda n, tab: (n, 0, 0)),
            ],
            scratch_shapes=[
                pltpu.VMEM((n_kv * length, dim), BF16),
                pltpu.VMEM((dim, n_kv * length), BF16),
                pltpu.VMEM((1, block), F32),
                pltpu.VMEM((1, block), F32),
                pltpu.VMEM((dim, block), F32),
            ],
        ),
        out_shape=[
            jax.ShapeDtypeStruct((length, n_heads * dim), BF16),
            jax.ShapeDtypeStruct((n_heads, 1, length), F32),
        ],
        cost_estimate=pl.CostEstimate(flops=8 * pairs * dim, bytes_accessed=8 * length * width, transcendentals=pairs),
        name=f'attn_fwd_{chunk}',
    )(start, start.reshape(1, -1), qkv_chunks[chunk], *qkv_chunks[:n_kv], *qkv_chunks[:n_kv])


def attention_backward_kernel(chunk, last, block, start_tab, start_ref, lse_ref, q_ref, do_ref, o_ref, *refs):
    n_kv = chunk + 1
    k_refs, v_refs, refs = refs[:n_kv], refs[n_kv:2 * n_kv], refs[2 * n_kv:]
    if not last:
        dk_in, dv_in, refs = refs[0], refs[1], refs[2:]
    dqkv_ref, refs = refs[0], refs[1:]
    if chunk:
        dk_out, dv_out, refs = refs[0], refs[1], refs[2:]
    k_all, v_all, k_t, dk_sum, dv_sum, dq_t = refs
    length, dim = q_ref.shape
    scale = dim ** -0.5
    scale2 = scale * LOG2_E
    for i in range(n_kv):
        rows = slice(i * length, (i + 1) * length)
        k_all[rows, :] = k_refs[i][...]
        v_all[rows, :] = v_refs[i][...]
        k_t[:, rows] = k_refs[i][...].T
    if last:
        dk_sum[...] = jnp.zeros(dk_sum.shape, F32)
        dv_sum[...] = jnp.zeros(dv_sum.shape, F32)
    else:
        dk_sum[...] = dk_in[...]
        dv_sum[...] = dv_in[...]
    for sub in range(length // block):
        rows = slice(sub * block, (sub + 1) * block)
        q0 = chunk * length + sub * block
        q_blk = q_ref[rows, :]
        do_blk = do_ref[rows, :]
        q_t = q_blk.T
        do_t = do_blk.T
        delta = jnp.sum((do_blk.astype(F32) * o_ref[rows, :].astype(F32)).T, axis=0, keepdims=True)
        lse = lse_ref[0, :, rows]
        starts = start_ref[:, rows]
        last_start = start_tab[q0 + block - 1]
        dq_t[...] = jnp.zeros(dq_t.shape, F32)

        def step(j, masked):
            k0 = pl.multiple_of(j * block, block)
            keys = pl.ds(k0, block)
            scores = dot32(k_all[keys, :], q_t, 1, 0)
            prob = jnp.exp2(scores * scale2 - lse)
            if masked:
                k_pos = k0 + lax.broadcasted_iota(jnp.int32, (block, block), 0)
                q_pos = q0 + lax.broadcasted_iota(jnp.int32, (block, block), 1)
                prob = jnp.where((k_pos <= q_pos) & (k_pos >= starts), prob, 0.0)
            d_prob = dot32(v_all[keys, :], do_t, 1, 0)
            d_score = (prob * (d_prob - delta)).astype(BF16)
            dv_sum[keys, :] += dot32(prob.astype(BF16), do_blk, 1, 0)
            dk_sum[keys, :] += dot32(d_score, q_blk, 1, 0)
            dq_t[...] += dot32(k_t[:, keys], d_score, 1, 0)

        def body(j, carry):
            needs_mask = (j * block + block - 1 > q0) | (j * block < last_start)
            pl.when(needs_mask)(lambda: step(j, True))
            pl.when(jnp.logical_not(needs_mask))(lambda: step(j, False))
            return carry

        lax.fori_loop(start_tab[q0] // block, q0 // block + 1, body, 0)
        dqkv_ref[rows, :dim] = (dq_t[...] * scale).T.astype(BF16)
    own = slice(chunk * length, n_kv * length)
    dqkv_ref[:, dim:2 * dim] = (dk_sum[own, :] * scale).astype(BF16)
    dqkv_ref[:, 2 * dim:] = dv_sum[own, :].astype(BF16)
    if chunk:
        dk_out[...] = dk_sum[:chunk * length, :]
        dv_out[...] = dv_sum[:chunk * length, :]


def attention_backward(chunk, last, block, n_heads, start, qkv_chunks, lse, d_attn, attn_out, sums):
    length, width = qkv_chunks[0].shape
    dim = width // (3 * n_heads)
    n_kv = chunk + 1
    spec = lambda part: pl.BlockSpec((length, dim), lambda n, tab: (0, 3 * n + part))
    head = lambda rows: pl.BlockSpec((rows, dim), lambda n, tab: (0, n))
    pairs = n_heads * length * (chunk * length + length // 2)
    out_specs = [pl.BlockSpec((length, 3 * dim), lambda n, tab: (0, n))]
    out_shape = [jax.ShapeDtypeStruct((length, width), BF16)]
    if chunk:
        out_specs += [head(chunk * length)] * 2
        out_shape += [jax.ShapeDtypeStruct((chunk * length, n_heads * dim), F32)] * 2
    outs = pl.pallas_call(
        functools.partial(attention_backward_kernel, chunk, last, block),
        grid_spec=pltpu.PrefetchScalarGridSpec(
            num_scalar_prefetch=1,
            grid=(n_heads,),
            in_specs=[
                pl.BlockSpec((1, length), lambda n, tab: (0, chunk)),
                pl.BlockSpec((1, 1, length), lambda n, tab: (n, 0, 0)),
                spec(0), head(length), head(length),
            ] + [spec(1)] * n_kv + [spec(2)] * n_kv + ([] if last else [head(n_kv * length)] * 2),
            out_specs=out_specs,
            scratch_shapes=[
                pltpu.VMEM((n_kv * length, dim), BF16),
                pltpu.VMEM((n_kv * length, dim), BF16),
                pltpu.VMEM((dim, n_kv * length), BF16),
                pltpu.VMEM((n_kv * length, dim), F32),
                pltpu.VMEM((n_kv * length, dim), F32),
                pltpu.VMEM((dim, block), F32),
            ],
        ),
        out_shape=out_shape,
        cost_estimate=pl.CostEstimate(flops=20 * pairs * dim, bytes_accessed=12 * length * width, transcendentals=pairs),
        name=f'attn_bwd_{chunk}',
    )(start, start.reshape(1, -1), lse, qkv_chunks[chunk], d_attn, attn_out, *qkv_chunks[:n_kv], *qkv_chunks[:n_kv], *sums)
    return outs[0], tuple(outs[1:])


class Order:
    def __init__(self):
        self.token = None

    def after(self, *args):
        if self.token is None:
            return args
        *args, self.token = lax.optimization_barrier((*args, self.token))
        return args

    def done(self, value):
        self.token = value
        return value


def solution(mesh):
    n_dev = mesh.shape['model']

    def local_step(x_in, seg_ids, gain_one, w_qkv, w_out, gain_two, w_up, w_down, d_y):
        seq_len, width = x_in.shape[1:]
        n_heads, head_dim = w_out.shape[:2]
        n_chunks = 4
        length = seq_len // n_chunks
        part = length // n_dev
        block = min(512, length)
        x_in, d_y, seg = x_in[0], d_y[0], seg_ids[0]
        w_out = w_out.reshape(n_heads * head_dim, width)
        me = lax.axis_index('model')
        core = me % 2
        n_chips = n_dev // 2
        chunks = range(n_chunks)
        order = Order()
        swap = [(i, i ^ 1) for i in range(n_dev)]
        same_core = [[2 * i + k for i in range(n_chips)] for k in range(2)]

        def chunk_of(array, c):
            return lax.slice_in_dim(array, c * length, (c + 1) * length, axis=0)

        def where(c):
            return (c * n_dev + me).astype(jnp.int32).reshape(1)

        def matmul(lhs, rhs, lhs_dim, rhs_dim, chunk=None):
            lhs, rhs = order.after(lhs, rhs)
            lhs = lhs if chunk is None else chunk_of(lhs, chunk)
            return order.done(dot32(lhs, rhs, lhs_dim, rhs_dim).astype(BF16))

        def rows_of_core(array, which):
            tiles = array.reshape(n_chips, 2, part, array.shape[-1])
            return lax.dynamic_index_in_dim(tiles, which, axis=1, keepdims=False).reshape(n_chips * part, -1)

        def send_half(lhs, rhs, rhs_dim):
            lhs, rhs = order.after(lhs, rhs)
            away = order.done(dot32(rows_of_core(lhs, 1 - core), rhs, 1, rhs_dim).astype(BF16))
            return lax.ppermute(away, 'model', swap)

        def sum_half(lhs, rhs, rhs_dim, arrived):
            lhs, rhs, arrived = order.after(lhs, rhs, arrived)
            both = order.done((dot32(rows_of_core(lhs, core), rhs, 1, rhs_dim) + arrived.astype(F32)).astype(BF16))
            return lax.psum_scatter(both, 'model', scatter_dimension=0, axis_index_groups=same_core, tiled=True)

        start = jnp.sum((seg[None, :] < seg[:, None]).astype(jnp.int32), axis=1)
        normed_one = order.done(norm_rows(x_in, gain_one, 0, length))

        qkv, attn, lse = [], [], []
        sent, total = {}, {}
        resid, normed_two, full_two, d_gelu, gelu_out, d_up, y_rows = {}, {}, {}, {}, {}, {}, {}
        d_resid, d_resid_full, d_gain_two, d_qkv, d_x_rows, d_gain_one = {}, {}, {}, {}, {}, {}
        sums = ()

        def qkv_in(c):
            qkv.append(matmul(normed_one, w_qkv, 1, 0, c))

        def attention_in(c):
            chunk_qkv = [*qkv[:c], order.after(qkv[c])[0]]
            attn_c, lse_c = attention_forward(c, block, n_heads, start, chunk_qkv)
            attn.append(order.done(attn_c))
            lse.append(lse_c)
            if c:
                sent['one', c] = send_half(attn_c, w_out, 0)
            else:
                total['one', c] = lax.psum_scatter(matmul(attn_c, w_out, 1, 0), 'model', scatter_dimension=0, tiled=True)

        def out_proj(c):
            total['one', c] = sum_half(attn[c], w_out, 0, sent['one', c])

        def second_norm(c):
            (summed,) = order.after(total['one', c])
            resid[c], normed_two[c] = add_norm(where(c), x_in, summed, gain_two)
            order.done(normed_two[c])

        def gelu_back(c):
            d_gelu[c] = matmul(d_y, w_down, 1, 1, c)

        def up(c):
            up_proj = matmul(*full_two[c][:1], w_up, 1, 0, full_two[c][1])
            gelu_c, gelu_pull = jax.vjp(gelu_tanh, up_proj)
            gelu_out[c], d_up[c] = lax.optimization_barrier((gelu_c, gelu_pull(d_gelu[c])[0]))
            order.done(d_up[c])

        def down_send(c):
            sent['two', c] = send_half(gelu_out[c], w_down, 0)

        def down(c):
            total['two', c] = sum_half(gelu_out[c], w_down, 0, sent['two', c])

        def finish_y(c):
            (summed,) = order.after(total['two', c])
            y_rows[c] = order.done((resid[c].astype(F32) + summed.astype(F32)).astype(BF16))

        def norm_two_send(c):
            sent['norm_two', c] = send_half(d_up[c], w_up, 1)

        def norm_two(c):
            total['norm_two', c] = sum_half(d_up[c], w_up, 1, sent['norm_two', c])

        def second_norm_back(c):
            (summed,) = order.after(total['norm_two', c])
            d_resid[c], d_gain_two[c] = norm_back(where(c), resid[c], d_y, summed, gain_two)
            order.done(d_resid[c])

        d_attn = {}

        def attention_grad(c):
            d_attn[c] = matmul(d_resid_full[c][0], w_out, 1, 1, d_resid_full[c][1])

        def attention_back(c):
            nonlocal sums
            (d_out,) = order.after(d_attn[c])
            d_qkv[c], sums = attention_backward(c, c == n_chunks - 1, block, n_heads, start, qkv, lse[c], d_out, attn[c], sums)
            order.done(d_qkv[c])
            sent['norm_one', c] = send_half(d_qkv[c], w_qkv, 1)

        def norm_one(c):
            total['norm_one', c] = sum_half(d_qkv[c], w_qkv, 1, sent['norm_one', c])

        def first_norm_back(c):
            (summed,) = order.after(total['norm_one', c])
            d_x_rows[c], d_gain_one[c] = norm_back(where(c), x_in, d_resid[c], summed, gain_one)
            order.done(d_x_rows[c])

        def joined(parts, which=chunks):
            if len(which) == 1:
                return parts[which[0]]
            return order.done(jnp.concatenate(order.after(*(parts[c] for c in which)), axis=0))

        def weight_grad(*pairs):
            summed = None
            for lhs, rhs in pairs:
                term = dot32(*order.after(lhs, rhs), 0, 0)
                summed = order.done(term if summed is None else summed + term)
            return order.done(summed.astype(BF16))

        def gather(rows, which):
            if len(which) == 1:
                return lax.all_gather(rows[which[0]], 'model', axis=0, tiled=True)
            stacked = jnp.stack([rows[c] for c in which])
            return lax.all_gather(stacked, 'model', axis=1, tiled=True).reshape(len(which) * length, width)

        def share(rows, full, which):
            array = gather(rows, which)
            for i, c in enumerate(which):
                full[c] = (array, i)
            return array

        qkv_in(0)
        attention_in(0)
        normed_one = order.done(norm_rows(x_in, gain_one, length, seq_len, order.after(normed_one)[0]))
        qkv_in(1)
        attention_in(1)
        second_norm(0)
        two_0 = share(normed_two, full_two, [0])
        qkv_in(2)
        out_proj(1)
        attention_in(2)
        qkv_in(3)
        out_proj(2)
        second_norm(1)
        two_1 = share(normed_two, full_two, [1])
        attention_in(3)
        gelu_back(0)
        out_proj(3)
        up(0)
        gelu_back(1)
        second_norm(2)
        down_send(0)
        up(1)
        down(0)
        second_norm(3)
        two_23 = share(normed_two, full_two, [2, 3])
        down_send(1)
        gelu_back(2)
        down(1)
        gelu_back(3)
        up(2)
        down_send(2)
        finish_y(0)
        y_0 = gather(y_rows, [0])
        up(3)
        down(2)
        norm_two_send(3)
        gelu_all = joined(gelu_out)
        norm_two(3)
        norm_two_send(2)
        finish_y(1)
        y_out = order.done(place(order.after(y_0)[0], seq_len, 0))
        norm_two(2)
        norm_two_send(1)
        d_up_23 = joined(d_up, [2, 3])
        second_norm_back(3)
        norm_two(1)
        norm_two_send(0)
        second_norm_back(2)
        resid_23 = share(d_resid, d_resid_full, [2, 3])
        finish_y(2)
        norm_two(0)
        down_send(3)
        d_w_down = weight_grad((gelu_all, d_y))
        down(3)
        attention_grad(3)
        attention_back(3)
        second_norm_back(1)
        second_norm_back(0)
        resid_01 = share(d_resid, d_resid_full, [0, 1])
        attention_grad(2)
        norm_one(3)
        finish_y(3)
        y_late = gather(y_rows, [1, 2, 3])
        attention_back(2)
        attn_23 = joined(attn, [2, 3])
        norm_one(2)
        attention_grad(1)
        attention_back(1)
        attention_grad(0)
        norm_one(1)
        attention_back(0)
        d_qkv_all = joined(d_qkv)
        norm_one(0)
        y_out = order.done(place(order.after(y_late)[0], seq_len, length, y_out))
        first_norm_back(3)
        d_w_qkv = weight_grad((normed_one, d_qkv_all))
        first_norm_back(2)
        d_w_out = weight_grad((attn_23, resid_23), (joined(attn, [0, 1]), resid_01))
        first_norm_back(1)
        d_x_late = gather(d_x_rows, [1, 2, 3])
        first_norm_back(0)
        d_x_first = gather(d_x_rows, [0])
        gain_sums = order.done(jnp.concatenate(order.after(sum(d_gain_one[c] for c in chunks), sum(d_gain_two[c] for c in chunks))))
        d_gains = order.done(lax.psum(gain_sums, 'model').astype(BF16))
        d_w_up = weight_grad((two_0, d_up[0]), (two_1, d_up[1]), (two_23, d_up_23))
        d_x = order.done(place(order.after(d_x_late)[0], seq_len, length))
        d_x = place(order.after(d_x_first)[0], seq_len, 0, d_x)
        return y_out[None], d_x[None], d_w_qkv, d_w_out.reshape(n_heads, head_dim, width), d_w_up, d_w_down, d_gains[0], d_gains[1]

    in_specs = (P('data'), P('data'), P(), P(None, 'model'), P('model'), P(), P(None, 'model'), P('model'), P('data'))
    out_specs = (P('data'), P('data'), P('data', 'model'), P(('data', 'model')), P('data', 'model'), P(('data', 'model')), P('data'), P('data'))
    return jax.shard_map(local_step, mesh=mesh, in_specs=in_specs, out_specs=out_specs, check_vma=False)
```
